32 devices in a mesh: stn: 8 (over z, x), pts: 2 (over core), freq: 2 (over y).
Axes of the slice: x: 2, y: 2, z: 4, core: 2. Of those that a mesh axis runs over, the one named last changes fastest.
Arguments:
- greens: bfloat16 [2, 4, 2048, 4096], P(None, 'freq', 'stn', 'pts'), may hold values from -6 to 6
- noise_weights: bfloat16 [2, 4, 2048, 2048], P(None, 'freq', 'stn'), may hold values from -12 to 12, as said below
Outputs:
- kernel: float32 [4096], P('pts')
The draws below stay inside these ranges and needn't reach their ends.
Inputs may be any that keep to these rules, and one draw needn't show every extreme that they name: For every frequency, noise_weights[0] is symmetric and noise_weights[1] antisymmetric in the two station dimensions, so each frequency's matrix is Hermitian.
All inputs are finite; a program needn't handle non-finite values. Where the reference program divides by a largest or mean magnitude, that divisor is 1e-20 or more.
Results may differ from the reference program's by a relative error of at most 0.0003.
Values may be sent and summed in bfloat16 or wider, within the bound.
A program may use at most 192 MiB of HBM per device.

```python
import jax
import jax.numpy as jnp
from jax import lax

S = 2048
F = 4
P_SIZE = 4096


def draw_noise_weights(key, part):
    base = jax.random.fold_in(key, 11)
    key_real, key_imag = jax.random.split(base, 2)
    rough_real = jax.random.truncated_normal(key_real, -4.0, 4.0, (F, S, S), jnp.float32) * 0.5
    rough_imag = jax.random.truncated_normal(key_imag, -4.0, 4.0, (F, S, S), jnp.float32) * 0.5
    symmetric = (rough_real + jnp.swapaxes(rough_real, 1, 2)) * 0.7071
    antisymmetric = (rough_imag - jnp.swapaxes(rough_imag, 1, 2)) * 0.7071
    return jnp.stack([symmetric, antisymmetric]).astype(jnp.bfloat16)


def levels(own_key, shape, shards, least, high):
    def one(position, blocks):
        steps = jax.random.uniform(jax.random.fold_in(jax.random.fold_in(own_key, 6), position), (blocks,), jnp.float32, least / len(shards), high / len(shards))
        return jnp.repeat(jnp.exp(steps), shape[position] // blocks).reshape((-1,) + (1,) * (len(shape) - position - 1))

    factor_of = one(*shards[0])
    for cut in shards[1:]:
        factor_of = factor_of * one(*cut)
    return factor_of


def noise(key, dims, deviation, most, pieces=(), kind=jnp.bfloat16):
    level = levels(key, dims, pieces, -0.22, 0.18) if pieces else 1.0
    result = jax.random.normal(key, dims, jnp.float32) * deviation * level
    return jnp.minimum(jnp.maximum(result, -most), most).astype(kind)


def setup_inputs(seed: int = 0) -> dict:
    seeds = jax.random.split(jax.random.key(seed), 3)
    greens = noise(seeds[0], (2, F, S, P_SIZE), 1.0, 6.0, ((1, 2), (2, 8), (3, 2)))
    noise_weights = draw_noise_weights(jax.random.fold_in(seeds[2], 71), 0)
    return {"greens": greens, "noise_weights": noise_weights}


def per_frequency(operands):
    green_block, weight_block = operands
    product_real = jnp.dot(weight_block[0], green_block[0], preferred_element_type=jnp.float32) - jnp.dot(weight_block[1], green_block[1], preferred_element_type=jnp.float32)
    product_imag = jnp.dot(weight_block[0], green_block[1], preferred_element_type=jnp.float32) + jnp.dot(weight_block[1], green_block[0], preferred_element_type=jnp.float32)
    green_real = green_block[0].astype(jnp.float32)
    green_imag = green_block[1].astype(jnp.float32)
    return jnp.sum(green_real * product_real + green_imag * product_imag, axis=0)


def reference(greens, noise_weights):
    stacked = lax.map(per_frequency, (jnp.moveaxis(greens, 1, 0), jnp.moveaxis(noise_weights, 1, 0)))
    raw_kernel = jnp.sum(stacked, axis=0) / S
    largest = jnp.max(jnp.abs(raw_kernel))
    return raw_kernel / (largest + 1e-6)
```

```python
import functools

import jax
import jax.numpy as jnp
from jax import lax
from jax.experimental import pallas as pl
from jax.experimental.pallas import tpu as pltpu
from jax.sharding import PartitionSpec as P

MESH = pl.DeviceIdType.MESH
LANES = 128


def remote(src, dst, send_sem, recv_sem, target):
    return pltpu.make_async_remote_copy(
        src_ref=src, dst_ref=dst, send_sem=send_sem, recv_sem=recv_sem,
        device_id=target, device_id_type=MESH,
    )


def ring_kernel(
    n, n_freq, h, stations, chunk, nq, blocked,
    greens, weights, out,
    g_own, g_pair, near, far, w_own, w_pair, acc, red, max_out, max_in,
    own_sem, w_own_sem, pair_send, pair_recv, wp_send, wp_recv, sib_sem,
    in_send, in_recv, out_send, far_recv, red_send, red_recv, max_sem,
):
    m = n // 2
    side_len = m // 2
    sub = chunk // LANES
    half_rows = h // 2
    me = lax.axis_index("stn")
    core = lax.axis_index("pts")
    fq = lax.axis_index("freq")
    parity = lax.rem(me, 2)
    z = me // 2
    hi = (z >= side_len).astype(jnp.int32)
    edge = jnp.where(hi == 1, m - 1 - z, z)
    inward = jnp.where(hi == 1, -2, 2)
    inner = edge == side_len - 1
    s_base = hi * nq
    r_base = (1 - hi) * nq
    pair_dev = {"stn": me + 1 - 2 * parity}
    in_dev = {"stn": me + inward}
    out_dev = {"stn": me - inward}
    n_far = side_len * 2 * nq
    n_near = edge * 4 * nq
    n_near_max = (side_len - 1) * 4 * nq
    steps = max(n_far, n_near_max, 3 * nq + 1)
    catch_up = max((steps * 25) // 32, 3 * nq)
    per_step = -(-steps // (steps - catch_up))

    def columns(q):
        return pl.ds(pl.multiple_of(q * chunk, LANES), chunk)

    def w_src(freq, j, rows):
        if blocked:
            return weights.at[:, freq, j, rows, :]
        return weights.at[:, freq, rows, pl.ds(pl.multiple_of(j * h, LANES), h)]

    def global_block(e, opposite):
        low = jnp.where(opposite, 1 - hi, hi) == 0
        return jnp.where(low, e, m - 1 - e)

    def near_slot(receiver_edge, p, half, b, c):
        return ((p * 2 + half) * receiver_edge + (receiver_edge - 1 - b)) * nq + c

    def far_slot(p, b, c):
        return (p * side_len + (side_len - 1 - b)) * nq + c

    def send_inward(src, p, half, b, c):
        q = jnp.where(half == 0, s_base, r_base) + c

        if side_len > 1:
            @pl.when(jnp.logical_not(inner))
            def _():
                slot = near_slot(edge + 1, p, half, b, c)
                remote(src, near.at[b, p, q], in_send.at[slot], in_recv.at[slot], in_dev).start()

        @pl.when(jnp.logical_and(inner, half == 0))
        def _():
            slot = far_slot(p, b, c)
            remote(src, far.at[b, p, c], in_send.at[slot], far_recv.at[slot], in_dev).start()

    every_row = pl.ds(0, h)
    pair_rows = pl.ds(pl.multiple_of(core * half_rows, 8), half_rows)

    def pair_q(i):
        return jnp.where(i < nq, s_base + i, r_base + i - nq)

    def pair_copy(i):
        q = pair_q(i)
        return remote(
            greens.at[:, 1 - parity, :, columns(q)], g_pair.at[q],
            pair_send.at[i], pair_recv.at[i], pair_dev,
        )

    def w_pair_copy(j):
        return remote(
            w_src(1 - parity, j, pair_rows), w_pair.at[j, :, pair_rows, :],
            wp_send.at[j], wp_recv.at[j], pair_dev,
        )

    def sibling_copy(rows):
        return remote(
            w_pair.at[:, :, rows, :], w_pair.at[:, :, rows, :],
            sib_sem.at[0], sib_sem.at[1], {"pts": 1 - core},
        )

    def own_copy(q):
        return pltpu.make_async_copy(
            greens.at[:, parity, :, columns(q)], g_own.at[q], own_sem.at[q]
        )

    def w_own_copy(j):
        return pltpu.make_async_copy(w_src(parity, j, every_row), w_own.at[j], w_own_sem.at[j])

    @pl.loop(0, 2 * nq)
    def _(i):
        pair_copy(i).start()
        half = i // nq
        c = lax.rem(i, nq)
        send_inward(greens.at[:, parity, :, columns(pair_q(i))], 0, half, edge, c)
        own_copy(i).start()

    @pl.loop(0, n)
    def _(j):
        w_pair_copy(j).start()
        w_own_copy(j).start()

    acc[...] = jnp.zeros_like(acc)

    @pl.loop(0, 2 * nq)
    def _(q):
        own_copy(q).wait()

    @pl.loop(0, n)
    def _(j):
        w_own_copy(j).wait()

    def contribute(w, gi, gj, q, weight):
        for s in range(sub):
            part = slice(s * LANES, (s + 1) * LANES)
            both = jnp.concatenate([gj[0, :, part], gj[1, :, part]], axis=1)
            a = jnp.dot(w[0], both, preferred_element_type=jnp.float32)
            b = jnp.dot(w[1], both, preferred_element_type=jnp.float32)
            t = gi[0, :, part].astype(jnp.float32) * (a[:, :LANES] - b[:, LANES:])
            t = t + gi[1, :, part].astype(jnp.float32) * (a[:, LANES:] + b[:, :LANES])
            t = jnp.sum(t.reshape(h // 8, 8, LANES), axis=0)
            acc[q * sub + s] += t * weight

    def far_at(t):
        p = t // (side_len * nq)
        rest = lax.rem(t, side_len * nq)
        return p, side_len - 1 - rest // nq, lax.rem(rest, nq)

    def near_at(t):
        width = jnp.maximum(edge, 1) * nq
        p = t // (2 * width)
        half = lax.rem(t // width, 2)
        rest = lax.rem(t, width)
        return p, half, jnp.maximum(edge, 1) - 1 - rest // nq, lax.rem(rest, nq)

    def part_of(p):
        return jnp.where(p == 0, parity, 1 - parity)

    def far_work(t, w, g):
        p, b, c = far_at(t)
        q = r_base + c
        j = global_block(b, True) * 2 + part_of(p)
        contribute(w.at[j], g.at[q], far.at[b, p, c], q, 2.0)

    def near_work(t, w, g):
        p, half, b, c = near_at(t)
        q = jnp.where(half == 0, s_base, r_base) + c
        j = global_block(b, False) * 2 + part_of(p)
        contribute(w.at[j], g.at[q], near.at[b, p, q], q, 2.0)

    def far_wait(t):
        p, b, c = far_at(t)
        ref = far.at[b, p, c]
        remote(ref, ref, out_send.at[t], far_recv.at[t], in_dev).wait_recv()

        @pl.when(edge > 0)
        def _():
            remote(ref, ref, out_send.at[t], far_recv.at[t], out_dev).start()

    def near_wait(t):
        p, half, b, c = near_at(t)
        q = jnp.where(half == 0, s_base, r_base) + c
        ref = near.at[b, p, q]
        remote(ref, ref, in_send.at[t], in_recv.at[t], out_dev).wait_recv()
        send_inward(ref, p, half, b, c)

    @pl.loop(0, steps)
    def _(t):
        has_pair = jnp.logical_and(t >= nq, t < 3 * nq)

        @pl.when(has_pair)
        def _():
            i = t - nq
            pair_copy(i).wait_recv()
            send_inward(g_pair.at[pair_q(i)], 1, i // nq, edge, lax.rem(i, nq))

        @pl.when(t < n_far)
        def _():
            far_wait(t)

        if side_len > 1:
            @pl.when(t < n_near)
            def _():
                near_wait(t)

        @pl.when(t == catch_up - 1)
        def _():
            @pl.loop(0, n)
            def _(j):
                w_pair_copy(j).wait_recv()

            sibling_copy(pair_rows).start()

        @pl.when(t < 2 * nq)
        def _():
            contribute(w_own.at[2 * z + parity], g_own.at[t], g_own.at[t], t, 1.0)

        @pl.when(has_pair)
        def _():
            q = pair_q(t - nq)
            contribute(w_own.at[2 * z + 1 - parity], g_own.at[q], g_pair.at[q], q, 2.0)

        @pl.when(t < n_far)
        def _():
            far_work(t, w_own, g_own)

        if side_len > 1:
            @pl.when(t < n_near)
            def _():
                near_work(t, w_own, g_own)

        @pl.when(t == catch_up)
        def _():
            sibling_copy(pl.ds(pl.multiple_of((1 - core) * half_rows, 8), half_rows)).wait_recv()

        @pl.when(t >= catch_up)
        def _():
            first = (t - catch_up) * per_step

            @pl.loop(first, jnp.minimum(first + per_step, steps))
            def _(u):
                @pl.when(u < 2 * nq)
                def _():
                    contribute(w_pair.at[2 * z + 1 - parity], g_pair.at[u], g_pair.at[u], u, 1.0)

                @pl.when(u < n_far)
                def _():
                    far_work(u, w_pair, g_pair)

                if side_len > 1:
                    @pl.when(u < n_near)
                    def _():
                        near_work(u, w_pair, g_pair)

    total = n * n_freq
    rank = me * n_freq + fq
    red[rank] = jnp.sum(acc[...], axis=1) / stations

    def share_copy(k, source):
        target = lax.rem(rank + k, total)
        return remote(
            red.at[source], red.at[source], red_send.at[k - 1], red_recv.at[k - 1],
            {"stn": target // n_freq, "freq": lax.rem(target, n_freq)},
        )

    @pl.loop(1, total)
    def _(k):
        share_copy(k, rank).start()

    @pl.loop(1, total)
    def _(k):
        share_copy(k, lax.rem(rank - k + total, total)).wait_recv()

    raw = red[0]
    for d in range(1, total):
        raw = raw + red[d]
    max_out[...] = jnp.broadcast_to(jnp.max(jnp.abs(raw)), max_out.shape)
    max_copy = remote(max_out, max_in, max_sem.at[0], max_sem.at[1], {"pts": 1 - core})
    max_copy.start()

    @pl.loop(1, total)
    def _(k):
        share_copy(k, rank).wait_send()

    @pl.loop(0, 2 * nq)
    def _(i):
        pair_copy(i).wait_send()

    @pl.loop(0, n)
    def _(j):
        w_pair_copy(j).wait_send()

    sibling_copy(pair_rows).wait_send()
    ref = far.at[0, 0, 0]

    @pl.loop(0, jnp.where(inner, n_far, (edge + 1) * 4 * nq))
    def _(t):
        remote(ref, ref, in_send.at[t], far_recv.at[0], in_dev).wait_send()

    @pl.when(edge > 0)
    def _():
        @pl.loop(0, n_far)
        def _(t):
            remote(ref, ref, out_send.at[t], far_recv.at[0], out_dev).wait_send()

    max_copy.wait()
    largest = jnp.maximum(max_out[0:1, 0:1], max_in[0:1, 0:1])
    out[...] = raw / (largest + 1e-6)


def kernel_body(n, n_freq, greens, weights):
    _, _, h, points = greens.shape
    stations = weights.shape[3]
    half = points // 2
    chunk = LANES
    while chunk * 2 * h <= 32768 and half % (chunk * 2) == 0:
        chunk *= 2
    nq = half // chunk
    side_len = n // 4
    n_far = side_len * 2 * nq
    n_near = max(side_len - 1, 1) * 4 * nq
    blocked = h % LANES != 0
    if blocked:
        weights = weights.reshape(2, weights.shape[1], h, n, h).swapaxes(2, 3)
    dma = pltpu.SemaphoreType.DMA
    bf16, f32 = jnp.bfloat16, jnp.float32
    rows = points // LANES
    out = pl.pallas_call(
        functools.partial(ring_kernel, n, n_freq, h, stations, chunk, nq, blocked),
        out_shape=jax.ShapeDtypeStruct((rows, LANES), f32),
        in_specs=[pl.BlockSpec(memory_space=pl.ANY)] * 2,
        out_specs=pl.BlockSpec(memory_space=pltpu.VMEM),
        scratch_shapes=[
            pltpu.VMEM((2 * nq, 2, h, chunk), bf16),
            pltpu.VMEM((2 * nq, 2, h, chunk), bf16),
            pltpu.VMEM((max(side_len - 1, 1), 2, 2 * nq, 2, h, chunk), bf16),
            pltpu.VMEM((side_len, 2, nq, 2, h, chunk), bf16),
            pltpu.VMEM((n, 2, h, h), bf16),
            pltpu.VMEM((n, 2, h, h), bf16),
            pltpu.VMEM((rows, 8, LANES), f32),
            pltpu.VMEM((n * n_freq, rows, LANES), f32),
            pltpu.VMEM((8, LANES), f32),
            pltpu.VMEM((8, LANES), f32),
            dma((2 * nq,)), dma((n,)), dma((2 * nq,)), dma((2 * nq,)), dma((n,)), dma((n,)), dma((2,)),
            dma((max(n_near, n_far),)), dma((n_near,)), dma((n_far,)), dma((n_far,)),
            dma((n * n_freq - 1,)), dma((n * n_freq - 1,)), dma((2,)),
        ],
        compiler_params=pltpu.CompilerParams(
            has_side_effects=True, vmem_limit_bytes=60 * 1024 * 1024
        ),
    )(greens, weights)
    return out.reshape(points)


def passed_along(x, axis, by):
    size = lax.axis_size(axis)
    return lax.ppermute(x, axis, [(i, (i + by) % size) for i in range(size)])


def mixing_of(weights):
    negated = -weights[1]
    return jnp.stack([jnp.stack([weights[0], negated]), jnp.stack([weights[1], weights[0]])])


def body(greens, noise_weights):
    station_rows = greens.shape[2]
    stations = noise_weights.shape[3]
    device_index = lax.axis_index("stn")
    cycle_length = lax.axis_size("stn")
    mixing = mixing_of(noise_weights)

    def block_product(columns_start, arriving):
        block_rows = arriving.shape[2]
        weights_block = lax.dynamic_slice_in_dim(mixing, columns_start, block_rows, 4)
        return jnp.einsum(
            "ocfin,cfnx->ofix", weights_block, arriving, preferred_element_type=jnp.float32
        )

    half_way = cycle_length // 2
    diagonal = block_product(device_index * station_rows, greens)

    def advance(offset, loop_state):
        running, current = loop_state
        current = passed_along(current, "stn", -1)
        source = (device_index + offset) % cycle_length
        weight = jnp.where(offset == half_way, 1.0, 2.0).astype(jnp.float32)
        running = running + weight * block_product(source * station_rows, current)
        return (running, current)

    summed, current = lax.fori_loop(1, half_way + 1, advance, (diagonal, greens))
    green_real = greens[0].astype(jnp.float32)
    green_imag = greens[1].astype(jnp.float32)
    partial_kernel = (
        jnp.sum(green_real * summed[0] + green_imag * summed[1], axis=(0, 1)) / stations
    )
    raw_kernel = lax.psum(partial_kernel, "stn")
    raw_kernel = lax.psum(raw_kernel, "freq")
    largest = lax.pmax(jnp.max(jnp.abs(raw_kernel)), "pts")
    return raw_kernel / (largest + 1e-06)


def solution(mesh):
    n, cores, n_freq = mesh.shape["stn"], mesh.shape["pts"], mesh.shape["freq"]

    def either(greens, noise_weights):
        _, freqs, rows, points = greens.shape
        fits = n % 4 == 0 and cores == 2 and freqs == 2 and rows % 32 == 0 and points % (2 * LANES) == 0
        if fits:
            return kernel_body(n, n_freq, greens, noise_weights)
        return body(greens, noise_weights)

    in_specs = (P(None, "freq", "stn", "pts"), P(None, "freq", "stn", None))
    return jax.shard_map(either, mesh=mesh, in_specs=in_specs, out_specs=P("pts"), check_vma=False)
```

```python
import functools

import jax
import jax.numpy as jnp
from jax import lax
from jax.experimental import pallas as pl
from jax.experimental.pallas import tpu as pltpu
from jax.sharding import PartitionSpec as P

MESH = pl.DeviceIdType.MESH
LANES = 128


def remote(src, dst, send_sem, recv_sem, target):
    return pltpu.make_async_remote_copy(
        src_ref=src, dst_ref=dst, send_sem=send_sem, recv_sem=recv_sem,
        device_id=target, device_id_type=MESH,
    )


def ring_kernel(
    n, n_freq, h, stations, chunk, nq, blocked,
    greens, weights, out,
    g_own, g_pair, near, far, w_own, w_pair, acc, red, max_out, max_in,
    own_sem, w_own_sem, pair_send, pair_recv, wp_send, wp_recv, sib_sem,
    in_send, in_recv, out_send, far_recv, red_send, red_recv, max_sem, hello_sem, pair_hello,
):
    m = n // 2
    side_len = m // 2
    sub = chunk // LANES
    half_rows = h // 2
    me = lax.axis_index("stn")
    core = lax.axis_index("pts")
    fq = lax.axis_index("freq")
    parity = lax.rem(me, 2)
    z = me // 2
    hi = (z >= side_len).astype(jnp.int32)
    edge = jnp.where(hi == 1, m - 1 - z, z)
    inward = jnp.where(hi == 1, -2, 2)
    inner = edge == side_len - 1
    s_base = hi * nq
    r_base = (1 - hi) * nq
    pair_dev = {"stn": me + 1 - 2 * parity}
    in_dev = {"stn": me + inward}
    out_dev = {"stn": me - inward}
    n_far = side_len * 2 * nq
    n_near = edge * 4 * nq
    n_near_max = (side_len - 1) * 4 * nq
    steps = max(n_far, n_near_max, 3 * nq + 2)
    spread = side_len == 2
    catch_up = 2 * nq + 1 if spread else max((steps * 25) // 32, 3 * nq + 1)
    left = steps - catch_up
    per_step = -(-steps // (steps - catch_up))

    def columns(q):
        return pl.ds(pl.multiple_of(q * chunk, LANES), chunk)

    def w_src(freq, j, rows):
        if blocked:
            return weights.at[:, freq, j, rows, :]
        return weights.at[:, freq, rows, pl.ds(pl.multiple_of(j * h, LANES), h)]

    def global_block(e, opposite):
        low = jnp.where(opposite, 1 - hi, hi) == 0
        return jnp.where(low, e, m - 1 - e)

    def near_slot(receiver_edge, p, half, b, c):
        return ((p * 2 + half) * receiver_edge + (receiver_edge - 1 - b)) * nq + c

    def far_slot(p, b, c):
        return (p * side_len + (side_len - 1 - b)) * nq + c

    def send_inward(src, p, half, b, c):
        q = jnp.where(half == 0, s_base, r_base) + c

        if side_len > 1:
            @pl.when(jnp.logical_not(inner))
            def _():
                slot = near_slot(edge + 1, p, half, b, c)
                remote(src, near.at[b, p, q], in_send.at[slot], in_recv.at[slot], in_dev).start()

        @pl.when(jnp.logical_and(inner, half == 0))
        def _():
            slot = far_slot(p, b, c)
            remote(src, far.at[b, p, c], in_send.at[slot], far_recv.at[slot], in_dev).start()

    freq_dev = {"freq": n_freq - 1 - fq}
    barrier = pltpu.get_barrier_semaphore()
    up, down = z < m - 1, z > 0
    greeted = [pair_dev, {"pts": 1 - core}, freq_dev]

    def greet(sem, device):
        pl.semaphore_signal(sem, inc=1, device_id=device, device_id_type=MESH)

    def along_z(sem_down, sem_up):
        @pl.when(up)
        def _():
            greet(sem_up, {"stn": me + 2})

        @pl.when(down)
        def _():
            greet(sem_down, {"stn": me - 2})

    for device in greeted:
        greet(barrier, device)
    along_z(barrier, barrier)
    pl.semaphore_wait(barrier, len(greeted) + up.astype(jnp.int32) + down.astype(jnp.int32))

    def hello():
        @pl.loop(0, m - 1)
        def _(r):
            along_z(hello_sem.at[0, r], hello_sem.at[1, r])

            @pl.when(up)
            def _():
                pl.semaphore_wait(hello_sem.at[0, r], 1)

            @pl.when(down)
            def _():
                pl.semaphore_wait(hello_sem.at[1, r], 1)

        for i, device in enumerate((pair_dev, freq_dev)):
            greet(pair_hello.at[i], device)
            pl.semaphore_wait(pair_hello.at[i], 1)

    every_row = pl.ds(0, h)
    pair_rows = pl.ds(pl.multiple_of(core * half_rows, 8), half_rows)

    def pair_q(i):
        return jnp.where(i < nq, s_base + i, r_base + i - nq)

    def pair_copy(i):
        q = pair_q(i)
        return remote(
            greens.at[:, 1 - parity, :, columns(q)], g_pair.at[q],
            pair_send.at[i], pair_recv.at[i], pair_dev,
        )

    def w_pair_copy(j):
        return remote(
            w_src(1 - parity, j, pair_rows), w_pair.at[j, :, pair_rows, :],
            wp_send.at[j], wp_recv.at[j], pair_dev,
        )

    def sibling_copy(rows):
        return remote(
            w_pair.at[:, :, rows, :], w_pair.at[:, :, rows, :],
            sib_sem.at[0], sib_sem.at[1], {"pts": 1 - core},
        )

    def own_copy(q):
        return pltpu.make_async_copy(
            greens.at[:, parity, :, columns(q)], g_own.at[q], own_sem.at[q]
        )

    def w_own_copy(j):
        return pltpu.make_async_copy(w_src(parity, j, every_row), w_own.at[j], w_own_sem.at[j])

    @pl.loop(0, 2 * nq)
    def _(i):
        @pl.when(i < nq)
        def _():
            pair_copy(i).start()

        half = i // nq
        c = lax.rem(i, nq)
        send_inward(greens.at[:, parity, :, columns(pair_q(i))], 0, half, edge, c)
        own_copy(i).start()

    @pl.loop(0, n)
    def _(j):
        w_pair_copy(j).start()
        w_own_copy(j).start()

    @pl.loop(nq, 2 * nq)
    def _(i):
        pair_copy(i).start()

    hello()

    acc[...] = jnp.zeros_like(acc)

    @pl.loop(0, 2 * nq)
    def _(q):
        own_copy(q).wait()

    @pl.loop(0, n)
    def _(j):
        w_own_copy(j).wait()

    def contribute(w, gi, gj, q, weight):
        for s in range(sub):
            part = slice(s * LANES, (s + 1) * LANES)
            both = jnp.concatenate([gj[0, :, part], gj[1, :, part]], axis=1)
            ab = jnp.dot(w[...].reshape(2 * h, h), both, preferred_element_type=jnp.float32)
            a, b = ab[:h], ab[h:]
            t = gi[0, :, part].astype(jnp.float32) * (a[:, :LANES] - b[:, LANES:])
            t = t + gi[1, :, part].astype(jnp.float32) * (a[:, LANES:] + b[:, :LANES])
            t = jnp.sum(t.reshape(h // 8, 8, LANES), axis=0)
            acc[q * sub + s] += t * weight

    def far_at(t):
        p = t // (side_len * nq)
        rest = lax.rem(t, side_len * nq)
        return p, side_len - 1 - rest // nq, lax.rem(rest, nq)

    def near_at(t):
        width = jnp.maximum(edge, 1) * nq
        p = t // (2 * width)
        half = lax.rem(t // width, 2)
        rest = lax.rem(t, width)
        return p, half, jnp.maximum(edge, 1) - 1 - rest // nq, lax.rem(rest, nq)

    def part_of(p):
        return jnp.where(p == 0, parity, 1 - parity)

    def far_work(t, w, g):
        p, b, c = far_at(t)
        q = r_base + c
        j = global_block(b, True) * 2 + part_of(p)
        contribute(w.at[j], g.at[q], far.at[b, p, c], q, 2.0)

    def near_work(t, w, g):
        p, half, b, c = near_at(t)
        q = jnp.where(half == 0, s_base, r_base) + c
        j = global_block(b, False) * 2 + part_of(p)
        contribute(w.at[j], g.at[q], near.at[b, p, q], q, 2.0)

    def far_wait(t):
        p, b, c = far_at(t)
        ref = far.at[b, p, c]
        remote(ref, ref, out_send.at[t], far_recv.at[t], in_dev).wait_recv()

        @pl.when(edge > 0)
        def _():
            remote(ref, ref, out_send.at[t], far_recv.at[t], out_dev).start()

    def near_wait(t):
        p, half, b, c = near_at(t)
        q = jnp.where(half == 0, s_base, r_base) + c
        ref = near.at[b, p, q]
        remote(ref, ref, in_send.at[t], in_recv.at[t], out_dev).wait_recv()
        send_inward(ref, p, half, b, c)

    def newest(u):
        far_work(u, w_pair, g_pair)

        @pl.when(u < n_near)
        def _():
            near_work(u, w_pair, g_pair)

    @pl.loop(0, steps)
    def _(t):
        has_pair = jnp.logical_and(jnp.logical_and(t >= nq, t <= 3 * nq), t != 2 * nq)
        turn = t - nq - (t > 2 * nq).astype(jnp.int32)

        @pl.when(has_pair)
        def _():
            i = turn
            pair_copy(i).wait_recv()
            send_inward(g_pair.at[pair_q(i)], 1, i // nq, edge, lax.rem(i, nq))

        @pl.when(t < n_far)
        def _():
            far_wait(t)

        if side_len > 1:
            @pl.when(t < n_near)
            def _():
                near_wait(t)

        @pl.when(t == catch_up - 1)
        def _():
            @pl.loop(0, n)
            def _(j):
                w_pair_copy(j).wait_recv()

            sibling_copy(pair_rows).start()

        @pl.when(t < 2 * nq)
        def _():
            contribute(w_own.at[2 * z + parity], g_own.at[t], g_own.at[t], t, 1.0)

        @pl.when(has_pair)
        def _():
            q = pair_q(turn)
            contribute(w_own.at[2 * z + 1 - parity], g_own.at[q], g_pair.at[q], q, 2.0)

        @pl.when(t < n_far)
        def _():
            far_work(t, w_own, g_own)

        if side_len > 1:
            @pl.when(t < n_near)
            def _():
                near_work(t, w_own, g_own)

        @pl.when(t == catch_up)
        def _():
            sibling_copy(pl.ds(pl.multiple_of((1 - core) * half_rows, 8), half_rows)).wait_recv()

        @pl.when(t >= catch_up)
        def _():
            first = (t - catch_up) * per_step
            last = jnp.minimum(first + per_step, steps)
            if spread:
                first = ((t - catch_up) * 2 * nq) // left
                last = ((t - catch_up + 1) * 2 * nq) // left

            @pl.loop(first, last)
            def _(u):
                @pl.when(u < 2 * nq)
                def _():
                    q = pair_q(u)
                    contribute(w_pair.at[2 * z + 1 - parity], g_pair.at[q], g_pair.at[q], q, 1.0)

                if spread:
                    far_work(lax.rem(u, side_len) * nq + u // side_len, w_pair, g_pair)
                else:
                    @pl.when(u < n_far)
                    def _():
                        far_work(u, w_pair, g_pair)

                if side_len > 1:
                    @pl.when(u < n_near)
                    def _():
                        near_work(u, w_pair, g_pair)

            if spread:
                newest(t - 1)

    if spread:
        newest(steps - 1)

    total = n * n_freq
    rank = me * n_freq + fq
    red[rank] = jnp.sum(acc[...], axis=1) / stations

    def share_copy(k, source):
        target = lax.rem(rank + k, total)
        return remote(
            red.at[source], red.at[source], red_send.at[k - 1], red_recv.at[k - 1],
            {"stn": target // n_freq, "freq": lax.rem(target, n_freq)},
        )

    @pl.loop(1, total)
    def _(k):
        share_copy(k, rank).start()

    @pl.loop(1, total)
    def _(k):
        share_copy(k, lax.rem(rank - k + total, total)).wait_recv()

    raw = red[0]
    for d in range(1, total):
        raw = raw + red[d]
    max_out[...] = jnp.broadcast_to(jnp.max(jnp.abs(raw)), max_out.shape)
    max_copy = remote(max_out, max_in, max_sem.at[0], max_sem.at[1], {"pts": 1 - core})
    max_copy.start()

    @pl.loop(1, total)
    def _(k):
        share_copy(k, rank).wait_send()

    @pl.loop(0, 2 * nq)
    def _(i):
        pair_copy(i).wait_send()

    @pl.loop(0, n)
    def _(j):
        w_pair_copy(j).wait_send()

    sibling_copy(pair_rows).wait_send()
    ref = far.at[0, 0, 0]

    @pl.loop(0, jnp.where(inner, n_far, (edge + 1) * 4 * nq))
    def _(t):
        remote(ref, ref, in_send.at[t], far_recv.at[0], in_dev).wait_send()

    @pl.when(edge > 0)
    def _():
        @pl.loop(0, n_far)
        def _(t):
            remote(ref, ref, out_send.at[t], far_recv.at[0], out_dev).wait_send()

    max_copy.wait()
    largest = jnp.maximum(max_out[0:1, 0:1], max_in[0:1, 0:1])
    out[...] = raw / (largest + 1e-6)


def kernel_body(n, n_freq, greens, weights):
    _, _, h, points = greens.shape
    stations = weights.shape[3]
    half = points // 2
    chunk = LANES
    while chunk * 2 * h <= 32768 and half % (chunk * 2) == 0:
        chunk *= 2
    nq = half // chunk
    side_len = n // 4
    n_far = side_len * 2 * nq
    n_near = max(side_len - 1, 1) * 4 * nq
    blocked = h % LANES != 0
    if blocked:
        weights = weights.reshape(2, weights.shape[1], h, n, h).swapaxes(2, 3)
    dma = pltpu.SemaphoreType.DMA
    bf16, f32 = jnp.bfloat16, jnp.float32
    rows = points // LANES
    out = pl.pallas_call(
        functools.partial(ring_kernel, n, n_freq, h, stations, chunk, nq, blocked),
        out_shape=jax.ShapeDtypeStruct((rows, LANES), f32),
        in_specs=[pl.BlockSpec(memory_space=pl.ANY)] * 2,
        out_specs=pl.BlockSpec(memory_space=pltpu.VMEM),
        scratch_shapes=[
            pltpu.VMEM((2 * nq, 2, h, chunk), bf16),
            pltpu.VMEM((2 * nq, 2, h, chunk), bf16),
            pltpu.VMEM((max(side_len - 1, 1), 2, 2 * nq, 2, h, chunk), bf16),
            pltpu.VMEM((side_len, 2, nq, 2, h, chunk), bf16),
            pltpu.VMEM((n, 2, h, h), bf16),
            pltpu.VMEM((n, 2, h, h), bf16),
            pltpu.VMEM((rows, 8, LANES), f32),
            pltpu.VMEM((n * n_freq, rows, LANES), f32),
            pltpu.VMEM((8, LANES), f32),
            pltpu.VMEM((8, LANES), f32),
            dma((2 * nq,)), dma((n,)), dma((2 * nq,)), dma((2 * nq,)), dma((n,)), dma((n,)), dma((2,)),
            dma((max(n_near, n_far),)), dma((n_near,)), dma((n_far,)), dma((n_far,)),
            dma((n * n_freq - 1,)), dma((n * n_freq - 1,)), dma((2,)),
            pltpu.SemaphoreType.REGULAR((2, n // 2 - 1)), pltpu.SemaphoreType.REGULAR((2,)),
        ],
        compiler_params=pltpu.CompilerParams(
            collective_id=0, has_side_effects=True, vmem_limit_bytes=60 * 1024 * 1024
        ),
    )(greens, weights)
    return out.reshape(points)


def passed_along(x, axis, by):
    size = lax.axis_size(axis)
    return lax.ppermute(x, axis, [(i, (i + by) % size) for i in range(size)])


def mixing_of(weights):
    negated = -weights[1]
    return jnp.stack([jnp.stack([weights[0], negated]), jnp.stack([weights[1], weights[0]])])


def body(greens, noise_weights):
    station_rows = greens.shape[2]
    stations = noise_weights.shape[3]
    device_index = lax.axis_index("stn")
    cycle_length = lax.axis_size("stn")
    mixing = mixing_of(noise_weights)

    def block_product(columns_start, arriving):
        block_rows = arriving.shape[2]
        weights_block = lax.dynamic_slice_in_dim(mixing, columns_start, block_rows, 4)
        return jnp.einsum(
            "ocfin,cfnx->ofix", weights_block, arriving, preferred_element_type=jnp.float32
        )

    half_way = cycle_length // 2
    diagonal = block_product(device_index * station_rows, greens)

    def advance(offset, loop_state):
        running, current = loop_state
        current = passed_along(current, "stn", -1)
        source = (device_index + offset) % cycle_length
        weight = jnp.where(offset == half_way, 1.0, 2.0).astype(jnp.float32)
        running = running + weight * block_product(source * station_rows, current)
        return (running, current)

    summed, current = lax.fori_loop(1, half_way + 1, advance, (diagonal, greens))
    green_real = greens[0].astype(jnp.float32)
    green_imag = greens[1].astype(jnp.float32)
    partial_kernel = (
        jnp.sum(green_real * summed[0] + green_imag * summed[1], axis=(0, 1)) / stations
    )
    raw_kernel = lax.psum(partial_kernel, "stn")
    raw_kernel = lax.psum(raw_kernel, "freq")
    largest = lax.pmax(jnp.max(jnp.abs(raw_kernel)), "pts")
    return raw_kernel / (largest + 1e-06)


def solution(mesh):
    n, cores, n_freq = mesh.shape["stn"], mesh.shape["pts"], mesh.shape["freq"]

    def either(greens, noise_weights):
        _, freqs, rows, points = greens.shape
        fits = n % 4 == 0 and cores == 2 and freqs == 2 and n_freq == 2 and rows % 32 == 0 and points % (2 * LANES) == 0
        if fits:
            return kernel_body(n, n_freq, greens, noise_weights)
        return body(greens, noise_weights)

    in_specs = (P(None, "freq", "stn", "pts"), P(None, "freq", "stn", None))
    return jax.shard_map(either, mesh=mesh, in_specs=in_specs, out_specs=P("pts"), check_vma=False)
```

```python
import functools

import jax
import jax.numpy as jnp
from jax import lax
from jax.experimental import pallas as pl
from jax.experimental.pallas import tpu as pltpu
from jax.sharding import PartitionSpec as P

MESH = pl.DeviceIdType.MESH
LANES = 128


def remote(src, dst, send_sem, recv_sem, target):
    return pltpu.make_async_remote_copy(
        src_ref=src, dst_ref=dst, send_sem=send_sem, recv_sem=recv_sem,
        device_id=target, device_id_type=MESH,
    )


def ring_kernel(
    n, n_freq, h, stations, chunk, nq, blocked,
    greens, weights, out,
    g_own, g_pair, near, far, w_own, w_pair, acc, red, max_out, max_in,
    own_sem, w_own_sem, pair_send, pair_recv, wp_send, wp_recv, sib_sem,
    in_send, in_recv, out_send, far_recv, red_send, red_recv, max_sem, hello_sem, pair_hello,
):
    m = n // 2
    side_len = m // 2
    sub = chunk // LANES
    half_rows = h // 2
    me = lax.axis_index("stn")
    core = lax.axis_index("pts")
    fq = lax.axis_index("freq")
    parity = lax.rem(me, 2)
    z = me // 2
    hi = (z >= side_len).astype(jnp.int32)
    edge = jnp.where(hi == 1, m - 1 - z, z)
    inward = jnp.where(hi == 1, -2, 2)
    inner = edge == side_len - 1
    s_base = hi * nq
    r_base = (1 - hi) * nq
    pair_dev = {"stn": me + 1 - 2 * parity}
    in_dev = {"stn": me + inward}
    out_dev = {"stn": me - inward}
    n_far = side_len * 2 * nq
    n_near = edge * 4 * nq
    n_near_max = (side_len - 1) * 4 * nq
    steps = max(n_far, n_near_max, 3 * nq + 2)
    spread = side_len == 2
    catch_up = 2 * nq + 1 if spread else max((steps * 25) // 32, 3 * nq + 1)
    left = steps - catch_up
    per_step = -(-steps // (steps - catch_up))

    def columns(q):
        return pl.ds(pl.multiple_of(q * chunk, LANES), chunk)

    def w_src(freq, j, rows):
        if blocked:
            return weights.at[:, freq, j, rows, :]
        return weights.at[:, freq, rows, pl.ds(pl.multiple_of(j * h, LANES), h)]

    def global_block(e, opposite):
        low = jnp.where(opposite, 1 - hi, hi) == 0
        return jnp.where(low, e, m - 1 - e)

    def near_slot(receiver_edge, p, half, b, c):
        return ((p * 2 + half) * receiver_edge + (receiver_edge - 1 - b)) * nq + c

    def far_slot(p, b, c):
        return (p * side_len + (side_len - 1 - b)) * nq + c

    def piece(k):
        return pl.ds(k * half_rows, half_rows)

    def send_inward(src, p, half, b, c):
        q = jnp.where(half == 0, s_base, r_base) + c

        if side_len > 1:
            @pl.when(jnp.logical_not(inner))
            def _():
                slot = near_slot(edge + 1, p, half, b, c)
                remote(src, near.at[b, p, q], in_send.at[slot, 0], in_recv.at[slot], in_dev).start()

        @pl.when(jnp.logical_and(inner, half == 0))
        def _():
            slot = far_slot(p, b, c)
            for k in range(2):
                remote(
                    src.at[:, piece(k), :], far.at[b, p, c, :, piece(k), :],
                    in_send.at[slot, k], far_recv.at[slot, k], in_dev,
                ).start()

    freq_dev = {"freq": n_freq - 1 - fq}
    barrier = pltpu.get_barrier_semaphore()
    up, down = z < m - 1, z > 0
    greeted = [pair_dev, {"pts": 1 - core}, freq_dev]

    def greet(sem, device):
        pl.semaphore_signal(sem, inc=1, device_id=device, device_id_type=MESH)

    def along_z(sem_down, sem_up):
        @pl.when(up)
        def _():
            greet(sem_up, {"stn": me + 2})

        @pl.when(down)
        def _():
            greet(sem_down, {"stn": me - 2})

    for device in greeted:
        greet(barrier, device)
    along_z(barrier, barrier)
    pl.semaphore_wait(barrier, len(greeted) + up.astype(jnp.int32) + down.astype(jnp.int32))

    def hello():
        @pl.loop(0, m - 1)
        def _(r):
            along_z(hello_sem.at[0, r], hello_sem.at[1, r])

            @pl.when(up)
            def _():
                pl.semaphore_wait(hello_sem.at[0, r], 1)

            @pl.when(down)
            def _():
                pl.semaphore_wait(hello_sem.at[1, r], 1)

        for i, device in enumerate((pair_dev, freq_dev)):
            greet(pair_hello.at[i], device)
            pl.semaphore_wait(pair_hello.at[i], 1)

    every_row = pl.ds(0, h)
    pair_rows = pl.ds(pl.multiple_of(core * half_rows, 8), half_rows)

    def pair_q(i):
        return jnp.where(i < nq, s_base + i, r_base + i - nq)

    def pair_copy(i):
        q = pair_q(i)
        return remote(
            greens.at[:, 1 - parity, :, columns(q)], g_pair.at[q],
            pair_send.at[i], pair_recv.at[i], pair_dev,
        )

    def w_pair_copy(j):
        return remote(
            w_src(1 - parity, j, pair_rows), w_pair.at[j, :, pair_rows, :],
            wp_send.at[j], wp_recv.at[j], pair_dev,
        )

    def sibling_copy(rows):
        return remote(
            w_pair.at[:, :, rows, :], w_pair.at[:, :, rows, :],
            sib_sem.at[0], sib_sem.at[1], {"pts": 1 - core},
        )

    def own_copy(q):
        return pltpu.make_async_copy(
            greens.at[:, parity, :, columns(q)], g_own.at[q], own_sem.at[q]
        )

    def w_own_copy(j):
        return pltpu.make_async_copy(w_src(parity, j, every_row), w_own.at[j], w_own_sem.at[j])

    @pl.loop(0, 2 * nq)
    def _(i):
        @pl.when(i < nq)
        def _():
            pair_copy(i).start()

        half = i // nq
        c = lax.rem(i, nq)
        send_inward(greens.at[:, parity, :, columns(pair_q(i))], 0, half, edge, c)
        own_copy(i).start()

    @pl.loop(0, n)
    def _(j):
        w_pair_copy(j).start()
        w_own_copy(j).start()

    @pl.loop(nq, 2 * nq)
    def _(i):
        pair_copy(i).start()

    hello()

    acc[...] = jnp.zeros_like(acc)

    @pl.loop(0, 2 * nq)
    def _(q):
        own_copy(q).wait()

    @pl.loop(0, n)
    def _(j):
        w_own_copy(j).wait()

    def contribute(w, gi, gj, q, weight):
        for s in range(sub):
            part = slice(s * LANES, (s + 1) * LANES)
            both = jnp.concatenate([gj[0, :, part], gj[1, :, part]], axis=1)
            ab = jnp.dot(w[...].reshape(2 * h, h), both, preferred_element_type=jnp.float32)
            a, b = ab[:h], ab[h:]
            t = gi[0, :, part].astype(jnp.float32) * (a[:, :LANES] - b[:, LANES:])
            t = t + gi[1, :, part].astype(jnp.float32) * (a[:, LANES:] + b[:, :LANES])
            t = jnp.sum(t.reshape(h // 8, 8, LANES), axis=0)
            acc[q * sub + s] += t * weight

    def far_at(t):
        p = t // (side_len * nq)
        rest = lax.rem(t, side_len * nq)
        return p, side_len - 1 - rest // nq, lax.rem(rest, nq)

    def near_at(t):
        width = jnp.maximum(edge, 1) * nq
        p = t // (2 * width)
        half = lax.rem(t // width, 2)
        rest = lax.rem(t, width)
        return p, half, jnp.maximum(edge, 1) - 1 - rest // nq, lax.rem(rest, nq)

    def part_of(p):
        return jnp.where(p == 0, parity, 1 - parity)

    def far_work(t, w, g):
        p, b, c = far_at(t)
        q = r_base + c
        j = global_block(b, True) * 2 + part_of(p)
        contribute(w.at[j], g.at[q], far.at[b, p, c], q, 2.0)

    def near_work(t, w, g):
        p, half, b, c = near_at(t)
        q = jnp.where(half == 0, s_base, r_base) + c
        j = global_block(b, False) * 2 + part_of(p)
        contribute(w.at[j], g.at[q], near.at[b, p, q], q, 2.0)

    def far_wait(t):
        p, b, c = far_at(t)
        for k in range(2):
            ref = far.at[b, p, c, :, piece(k), :]
            remote(ref, ref, out_send.at[t, k], far_recv.at[t, k], in_dev).wait_recv()

            @pl.when(edge > 0)
            def _():
                remote(ref, ref, out_send.at[t, k], far_recv.at[t, k], out_dev).start()

    def near_wait(t):
        p, half, b, c = near_at(t)
        q = jnp.where(half == 0, s_base, r_base) + c
        ref = near.at[b, p, q]
        remote(ref, ref, in_send.at[t, 0], in_recv.at[t], out_dev).wait_recv()
        send_inward(ref, p, half, b, c)

    def newest(u):
        far_work(u, w_pair, g_pair)

        @pl.when(u < n_near)
        def _():
            near_work(u, w_pair, g_pair)

    @pl.loop(0, steps)
    def _(t):
        has_pair = jnp.logical_and(jnp.logical_and(t >= nq, t <= 3 * nq), t != 2 * nq)
        turn = t - nq - (t > 2 * nq).astype(jnp.int32)

        @pl.when(has_pair)
        def _():
            i = turn
            pair_copy(i).wait_recv()
            send_inward(g_pair.at[pair_q(i)], 1, i // nq, edge, lax.rem(i, nq))

        @pl.when(t < n_far)
        def _():
            far_wait(t)

        if side_len > 1:
            @pl.when(t < n_near)
            def _():
                near_wait(t)

        @pl.when(t == catch_up - 1)
        def _():
            @pl.loop(0, n)
            def _(j):
                w_pair_copy(j).wait_recv()

            sibling_copy(pair_rows).start()

        @pl.when(t < 2 * nq)
        def _():
            contribute(w_own.at[2 * z + parity], g_own.at[t], g_own.at[t], t, 1.0)

        @pl.when(has_pair)
        def _():
            q = pair_q(turn)
            contribute(w_own.at[2 * z + 1 - parity], g_own.at[q], g_pair.at[q], q, 2.0)

        @pl.when(t < n_far)
        def _():
            far_work(t, w_own, g_own)

        if side_len > 1:
            @pl.when(t < n_near)
            def _():
                near_work(t, w_own, g_own)

        @pl.when(t == catch_up)
        def _():
            sibling_copy(pl.ds(pl.multiple_of((1 - core) * half_rows, 8), half_rows)).wait_recv()

        @pl.when(t >= catch_up)
        def _():
            first = (t - catch_up) * per_step
            last = jnp.minimum(first + per_step, steps)
            if spread:
                first = ((t - catch_up) * 2 * nq) // left
                last = ((t - catch_up + 1) * 2 * nq) // left

            @pl.loop(first, last)
            def _(u):
                @pl.when(u < 2 * nq)
                def _():
                    q = pair_q(u)
                    contribute(w_pair.at[2 * z + 1 - parity], g_pair.at[q], g_pair.at[q], q, 1.0)

                if spread:
                    far_work(lax.rem(u, side_len) * nq + u // side_len, w_pair, g_pair)
                else:
                    @pl.when(u < n_far)
                    def _():
                        far_work(u, w_pair, g_pair)

                if side_len > 1:
                    @pl.when(u < n_near)
                    def _():
                        near_work(u, w_pair, g_pair)

            if spread:
                newest(t - 1)

    if spread:
        newest(steps - 1)

    total = n * n_freq
    rank = me * n_freq + fq
    red[rank] = jnp.sum(acc[...], axis=1) / stations

    def share_copy(k, source):
        target = lax.rem(rank + k, total)
        return remote(
            red.at[source], red.at[source], red_send.at[k - 1], red_recv.at[k - 1],
            {"stn": target // n_freq, "freq": lax.rem(target, n_freq)},
        )

    @pl.loop(1, total)
    def _(k):
        share_copy(k, rank).start()

    @pl.loop(1, total)
    def _(k):
        share_copy(k, lax.rem(rank - k + total, total)).wait_recv()

    raw = red[0]
    for d in range(1, total):
        raw = raw + red[d]
    max_out[...] = jnp.broadcast_to(jnp.max(jnp.abs(raw)), max_out.shape)
    max_copy = remote(max_out, max_in, max_sem.at[0], max_sem.at[1], {"pts": 1 - core})
    max_copy.start()

    @pl.loop(1, total)
    def _(k):
        share_copy(k, rank).wait_send()

    @pl.loop(0, 2 * nq)
    def _(i):
        pair_copy(i).wait_send()

    @pl.loop(0, n)
    def _(j):
        w_pair_copy(j).wait_send()

    sibling_copy(pair_rows).wait_send()
    whole = far.at[0, 0, 0]
    parts = [far.at[0, 0, 0, :, piece(k), :] for k in range(2)]

    @pl.when(inner)
    def _():
        @pl.loop(0, n_far)
        def _(t):
            for k in range(2):
                remote(parts[k], parts[k], in_send.at[t, k], far_recv.at[0, k], in_dev).wait_send()

    if side_len > 1:
        @pl.when(jnp.logical_not(inner))
        def _():
            @pl.loop(0, (edge + 1) * 4 * nq)
            def _(t):
                remote(whole, whole, in_send.at[t, 0], far_recv.at[0, 0], in_dev).wait_send()

    @pl.when(edge > 0)
    def _():
        @pl.loop(0, n_far)
        def _(t):
            for k in range(2):
                remote(parts[k], parts[k], out_send.at[t, k], far_recv.at[0, k], out_dev).wait_send()

    max_copy.wait()
    largest = jnp.maximum(max_out[0:1, 0:1], max_in[0:1, 0:1])
    out[...] = raw / (largest + 1e-6)


def kernel_body(n, n_freq, greens, weights):
    _, _, h, points = greens.shape
    stations = weights.shape[3]
    half = points // 2
    chunk = LANES
    while chunk * 2 * h <= 32768 and half % (chunk * 2) == 0:
        chunk *= 2
    nq = half // chunk
    side_len = n // 4
    n_far = side_len * 2 * nq
    n_near = max(side_len - 1, 1) * 4 * nq
    blocked = h % LANES != 0
    if blocked:
        weights = weights.reshape(2, weights.shape[1], h, n, h).swapaxes(2, 3)
    dma = pltpu.SemaphoreType.DMA
    bf16, f32 = jnp.bfloat16, jnp.float32
    rows = points // LANES
    out = pl.pallas_call(
        functools.partial(ring_kernel, n, n_freq, h, stations, chunk, nq, blocked),
        out_shape=jax.ShapeDtypeStruct((rows, LANES), f32),
        in_specs=[pl.BlockSpec(memory_space=pl.ANY)] * 2,
        out_specs=pl.BlockSpec(memory_space=pltpu.VMEM),
        scratch_shapes=[
            pltpu.VMEM((2 * nq, 2, h, chunk), bf16),
            pltpu.VMEM((2 * nq, 2, h, chunk), bf16),
            pltpu.VMEM((max(side_len - 1, 1), 2, 2 * nq, 2, h, chunk), bf16),
            pltpu.VMEM((side_len, 2, nq, 2, h, chunk), bf16),
            pltpu.VMEM((n, 2, h, h), bf16),
            pltpu.VMEM((n, 2, h, h), bf16),
            pltpu.VMEM((rows, 8, LANES), f32),
            pltpu.VMEM((n * n_freq, rows, LANES), f32),
            pltpu.VMEM((8, LANES), f32),
            pltpu.VMEM((8, LANES), f32),
            dma((2 * nq,)), dma((n,)), dma((2 * nq,)), dma((2 * nq,)), dma((n,)), dma((n,)), dma((2,)),
            dma((max(n_near, n_far), 2)), dma((n_near,)), dma((n_far, 2)), dma((n_far, 2)),
            dma((n * n_freq - 1,)), dma((n * n_freq - 1,)), dma((2,)),
            pltpu.SemaphoreType.REGULAR((2, n // 2 - 1)), pltpu.SemaphoreType.REGULAR((2,)),
        ],
        compiler_params=pltpu.CompilerParams(
            collective_id=0, has_side_effects=True, vmem_limit_bytes=60 * 1024 * 1024
        ),
    )(greens, weights)
    return out.reshape(points)


def passed_along(x, axis, by):
    size = lax.axis_size(axis)
    return lax.ppermute(x, axis, [(i, (i + by) % size) for i in range(size)])


def mixing_of(weights):
    negated = -weights[1]
    return jnp.stack([jnp.stack([weights[0], negated]), jnp.stack([weights[1], weights[0]])])


def body(greens, noise_weights):
    station_rows = greens.shape[2]
    stations = noise_weights.shape[3]
    device_index = lax.axis_index("stn")
    cycle_length = lax.axis_size("stn")
    mixing = mixing_of(noise_weights)

    def block_product(columns_start, arriving):
        block_rows = arriving.shape[2]
        weights_block = lax.dynamic_slice_in_dim(mixing, columns_start, block_rows, 4)
        return jnp.einsum(
            "ocfin,cfnx->ofix", weights_block, arriving, preferred_element_type=jnp.float32
        )

    half_way = cycle_length // 2
    diagonal = block_product(device_index * station_rows, greens)

    def advance(offset, loop_state):
        running, current = loop_state
        current = passed_along(current, "stn", -1)
        source = (device_index + offset) % cycle_length
        weight = jnp.where(offset == half_way, 1.0, 2.0).astype(jnp.float32)
        running = running + weight * block_product(source * station_rows, current)
        return (running, current)

    summed, current = lax.fori_loop(1, half_way + 1, advance, (diagonal, greens))
    green_real = greens[0].astype(jnp.float32)
    green_imag = greens[1].astype(jnp.float32)
    partial_kernel = (
        jnp.sum(green_real * summed[0] + green_imag * summed[1], axis=(0, 1)) / stations
    )
    raw_kernel = lax.psum(partial_kernel, "stn")
    raw_kernel = lax.psum(raw_kernel, "freq")
    largest = lax.pmax(jnp.max(jnp.abs(raw_kernel)), "pts")
    return raw_kernel / (largest + 1e-06)


def solution(mesh):
    n, cores, n_freq = mesh.shape["stn"], mesh.shape["pts"], mesh.shape["freq"]

    def either(greens, noise_weights):
        _, freqs, rows, points = greens.shape
        fits = n % 4 == 0 and cores == 2 and freqs == 2 and n_freq == 2 and rows % 32 == 0 and points % (2 * LANES) == 0
        if fits:
            return kernel_body(n, n_freq, greens, noise_weights)
        return body(greens, noise_weights)

    in_specs = (P(None, "freq", "stn", "pts"), P(None, "freq", "stn", None))
    return jax.shard_map(either, mesh=mesh, in_specs=in_specs, out_specs=P("pts"), check_vma=False)
```
